32 devices in a mesh: row: 4 (over y, core), col: 8 (over z, x).
Axes of the slice: x: 2, y: 2, z: 4, core: 2. Of those that a mesh axis runs over, the one named last changes fastest.
Arguments:
- vectors: bfloat16 [4, 8, 128, 384], P('row', 'col'), may hold values from -6 to 6
- near_blocks: bfloat16 [4, 8, 9, 384, 384], P('row', 'col'), may hold values from -0.15625 to 0.15625
- near_source: int32 [4, 8, 9], P('row', 'col'), may hold values from 0 to 8, each once within a row
- near_count: int32 [4, 8], P('row', 'col'), may hold values from 1 to 9
- basis_col: bfloat16 [4, 8, 64, 384], P('row', 'col'), may hold values from -0.3125 to 0.3125
- transfer_col: bfloat16 [4, 8, 64, 64], P('row', 'col'), may hold values from -0.25 to 0.25
- leaf_couple: bfloat16 [4, 8, 3, 5, 64, 64], P('row', 'col'), may hold values from -0.1875 to 0.1875
- coupling: bfloat16 [4, 4, 64, 64], P('row'), may hold values from -0.75 to 0.75
- distant_region_list: int32 [4, 4], P('row'), may hold values from 0 to 3, each once within a row
- transfer_row: bfloat16 [4, 8, 64, 64], P('row', 'col'), may hold values from -0.75 to 0.75
- basis_row: bfloat16 [4, 8, 64, 384], P('row', 'col'), may hold values from -0.75 to 0.75
Outputs:
- product: bfloat16 [4, 8, 128, 384], P('row', 'col')
The draws below stay inside these ranges and needn't reach their ends.
Inputs may be any that keep to these rules, and one draw needn't show every extreme that they name: `near_source`: the 9 slots of a leaf name the nine neighbourhood cells once each. Only the first near_count slots of a leaf are live. `distant_region_list`: each region's list names every region once.
All inputs are finite; a program needn't handle non-finite values.
Results may differ from the reference program's by a relative error of at most 0.013.
Values may be sent and summed in bfloat16 or wider, within the bound.
A program may use at most 64 MiB of HBM per device.

```python
import jax
import jax.numpy as jnp
from jax import lax

LEAF = 384
RANK = 64
NEAR = 9
VECS = 128
RFAR = 1
BAND = 5
N_ROW = 4
N_COL = 8


def touch_ends(array, key, least, high):
    place = [jax.random.randint(jax.random.fold_in(key, axis), (), 0, length) for axis, length in enumerate(array.shape)]
    main_axis = array.shape.index(max(array.shape))
    next_to = place[:main_axis] + [(place[main_axis] + 1) % array.shape[main_axis]] + place[main_axis + 1:]
    return array.at[tuple(place)].set(least).at[tuple(next_to)].set(high)


def steps_of(key, dims, shards, low, largest):
    level, own = 1.0, jax.random.fold_in(key, 6)
    for axis_at, shards_of in shards:
        heights = jnp.exp(jax.random.uniform(jax.random.fold_in(own, axis_at), (shards_of,), jnp.float32, low / len(shards), largest / len(shards)))
        level = level * jnp.repeat(heights, dims[axis_at] // shards_of).reshape([-1 if axis == axis_at else 1 for axis in range(len(dims))])
    return level


def normal_values(key, extent, width, limit, cuts=(), kind=jnp.bfloat16):
    values = width * jax.random.normal(key, extent, jnp.float32)
    if cuts:
        values = values * steps_of(key, extent, cuts, -0.22, 0.18)
    return jnp.clip(values, -limit, limit).astype(kind)


def setup_inputs(seed: int = 0) -> dict:
    splits = jax.random.split(jax.random.key(seed), 12)
    return {
        "vectors": normal_values(splits[0], (N_ROW, N_COL, VECS, LEAF), 1.0, 6.0, ((0, 4), (1, 8))),
        "near_blocks": normal_values(splits[1], (N_ROW, N_COL, NEAR, LEAF, LEAF), (LEAF * 4) ** -0.5, 0.15625, ((0, 4), (1, 8))),
        "near_source": jax.vmap(lambda own: jax.random.permutation(own, NEAR))(jax.random.split(splits[2], N_ROW * N_COL)).reshape((N_ROW, N_COL, NEAR)).astype(jnp.int32),
        "near_count": touch_ends(jax.random.randint(splits[3], (N_ROW, N_COL), 1, NEAR + 1), jax.random.fold_in(splits[3], 1), 1, NEAR).astype(jnp.int32),
        "basis_col": normal_values(splits[4], (N_ROW, N_COL, RANK, LEAF), LEAF ** -0.5, 0.3125, ((0, 4), (1, 8))),
        "transfer_col": normal_values(splits[5], (N_ROW, N_COL, RANK, RANK), (RANK * N_COL) ** -0.5, 0.25, ((0, 4), (1, 8))),
        "leaf_couple": normal_values(splits[6], (N_ROW, N_COL, 3, BAND, RANK, RANK), (RANK * 3 * BAND) ** -0.5, 0.1875, ((0, 4), (1, 8))),
        "coupling": normal_values(splits[7], (N_ROW, N_ROW, RANK, RANK), (RANK * RFAR) ** -0.5, 0.75, ((0, 4),)),
        "distant_region_list": jax.vmap(lambda own: jax.random.permutation(own, N_ROW))(jax.random.split(splits[8], N_ROW)).reshape((N_ROW, N_ROW)).astype(jnp.int32),
        "transfer_row": normal_values(splits[9], (N_ROW, N_COL, RANK, RANK), RANK ** -0.5, 0.75, ((0, 4), (1, 8))),
        "basis_row": normal_values(splits[10], (N_ROW, N_COL, RANK, LEAF), RANK ** -0.5, 0.75, ((0, 4), (1, 8))),
    }


def reference(vectors, near_blocks, near_source, near_count, basis_col, transfer_col, leaf_couple, coupling, distant_region_list, transfer_row, basis_row):
    upper_limit = lax.Precision.HIGHEST
    flat_vectors = vectors.reshape(N_ROW * N_COL, VECS, LEAF)
    row_identifiers = jnp.arange(N_ROW, dtype=jnp.int32)[:, None]
    col_ids = jnp.arange(N_COL, dtype=jnp.int32)[None, :]
    near = jnp.zeros((N_ROW, N_COL, VECS, LEAF), jnp.float32)
    for slot in range(NEAR):
        cell = near_source[:, :, slot]
        rows_src = (row_identifiers + cell // 3) % N_ROW
        cols_src = (col_ids + cell % 3) % N_COL
        flat = (rows_src * N_COL + cols_src).astype(jnp.int32)
        source = flat_vectors[flat].astype(jnp.float32)
        live = (near_count > slot).astype(jnp.float32)
        term = jnp.einsum("rcvp,rcpq->rcvq", source, near_blocks[:, :, slot].astype(jnp.float32), precision=upper_limit)
        near = near + live[:, :, None, None] * term
    incoming_leaf = jnp.einsum("rcvp,rckp->rcvk", vectors.astype(jnp.float32), basis_col.astype(jnp.float32), precision=upper_limit)
    band = jnp.zeros((N_ROW, N_COL, VECS, RANK), jnp.float32)
    for delta in range(3):
        for start_shift in range(BAND):
            shifted = jnp.roll(incoming_leaf, (-delta, -(3 + start_shift)), axis=(0, 1))
            band = band + jnp.einsum("rcvk,rckl->rcvl", shifted, leaf_couple[:, :, delta, start_shift].astype(jnp.float32), precision=upper_limit)
    incoming_region = jnp.einsum("rcvk,rckl->rvl", incoming_leaf, transfer_col.astype(jnp.float32), precision=upper_limit)
    region_ids = jnp.arange(N_ROW, dtype=jnp.int32)[:, None]
    far_mask = (((distant_region_list - region_ids) % N_ROW) >= 3).astype(jnp.float32)
    listed = incoming_region[distant_region_list] * far_mask[:, :, None, None]
    outgoing_region = jnp.einsum("ibne,iber->inr", listed, coupling.astype(jnp.float32), precision=upper_limit)
    leaf_out = band + jnp.einsum("rvk,rckl->rcvl", outgoing_region, transfer_row.astype(jnp.float32), precision=upper_limit)
    far = jnp.einsum("rcvk,rckq->rcvq", leaf_out, basis_row.astype(jnp.float32), precision=upper_limit)
    return (near + far).astype(jnp.bfloat16)
```

```python
import functools

import jax
import jax.numpy as jnp
from jax import lax
from jax.experimental import pallas as pl
from jax.experimental.pallas import tpu as pltpu
from jax.sharding import PartitionSpec as P

REACH = 3
MESH = pl.DeviceIdType.MESH
BF16 = jnp.bfloat16
F32 = jnp.float32


def dot(a, b, dims):
    return lax.dot_general(a, b, (dims, ((), ())), preferred_element_type=F32)


def kernel(
    rows,
    cols,
    source_ref,
    count_ref,
    list_ref,
    vectors_hbm,
    blocks_hbm,
    basis_col_hbm,
    transfer_col_hbm,
    couple_hbm,
    coupling_hbm,
    transfer_row_hbm,
    basis_row_hbm,
    out_ref,
    table,
    blocks,
    basis_col,
    transfer_col,
    couple,
    coupling,
    transfer_row,
    basis_row,
    leaf_send,
    up_send,
    leaf_buf,
    region_buf,
    local_sems,
    near_send_sems,
    near_recv_sems,
    group_sems,
):
    r, c = lax.axis_index("row"), lax.axis_index("col")
    band = cols - REACH

    def behind(d, e):
        return (lax.rem(r + rows - d, rows), lax.rem(c + cols - e, cols))

    barrier = pltpu.get_barrier_semaphore()
    if rows * cols <= 64:
        for k in range(1, rows * cols):
            pl.semaphore_signal(barrier, inc=1, device_id=behind(k // cols, k % cols), device_id_type=MESH)
    else:

        @pl.loop(1, rows * cols)
        def _(k):
            pl.semaphore_signal(
                barrier, inc=1, device_id=behind(k // cols, lax.rem(k, cols)), device_id_type=MESH
            )

    loads = [
        pltpu.make_async_copy(src, dst, local_sems.at[i])
        for i, (src, dst) in enumerate(
            [
                (vectors_hbm, table.at[0]),
                (basis_col_hbm, basis_col),
                (transfer_col_hbm, transfer_col),
                (blocks_hbm, blocks),
                (couple_hbm, couple),
                (coupling_hbm, coupling),
                (transfer_row_hbm, transfer_row),
                (basis_row_hbm, basis_row),
            ]
        )
    ]
    for load in loads:
        load.start()
    for load in loads[:3]:
        load.wait()
    leaf = dot(basis_col[...], table[0], ((1,), (1,)))
    leaf_low = leaf.astype(BF16)
    leaf_send[...] = leaf_low
    up_send[...] = dot(transfer_col[...], leaf_low, ((0,), (0,))).astype(BF16)

    pl.semaphore_wait(barrier, rows * cols - 1)

    def send(src, dst, send_sem, recv_sem, target):
        copy = pltpu.make_async_remote_copy(
            src_ref=src, dst_ref=dst, send_sem=send_sem, recv_sem=recv_sem,
            device_id=target, device_id_type=MESH,
        )
        copy.start()
        return copy

    for d in range(REACH, rows):
        for e in range(cols):
            send(up_send, region_buf.at[(d - REACH) * cols + e], group_sems.at[0], group_sems.at[1], behind(d, e))
    near = {}
    for d, e in ((2, 2), (2, 1), (1, 2), (1, 1), (0, 2), (2, 0), (1, 0), (0, 1)):
        cell = d * REACH + e
        near[cell] = send(
            table.at[0], table.at[cell], near_send_sems.at[cell], near_recv_sems.at[cell], behind(d, e)
        )
    for d in range(REACH):
        for j in range(band):
            send(leaf_send, leaf_buf.at[d * band + j], group_sems.at[2], group_sems.at[3], behind(d, REACH + j))

    for load in loads[3:]:
        load.wait()

    count = count_ref[0, 0]

    def term(cell):
        slot = jnp.int32(0)
        for s in range(source_ref.shape[0]):
            slot = jnp.where(source_ref[s] == cell, s, slot)
        source = table[cell]
        source = jnp.where(slot < count, source, jnp.zeros_like(source))
        return dot(source, blocks[slot], ((1,), (0,)))

    total = term(0)
    for cell in (1, 3, 2, 6, 4, 5, 7, 8):
        near[cell].wait_recv()
        total = total + term(cell)

    pltpu.make_async_copy(region_buf, region_buf, group_sems.at[1]).wait()
    region_out = None
    for d in range(REACH, rows):
        target = lax.rem(r + d, rows)
        slot = jnp.int32(0)
        for f in range(rows):
            slot = jnp.where(list_ref[f] == target, f, slot)
        region = jnp.sum(region_buf[pl.ds((d - REACH) * cols, cols)].astype(F32), axis=0)
        part = dot(coupling[slot], region.astype(BF16), ((0,), (0,)))
        region_out = part if region_out is None else region_out + part
    leaf_out = dot(transfer_row[...], region_out.astype(BF16), ((0,), (0,)))
    pltpu.make_async_copy(leaf_buf, leaf_buf, group_sems.at[3]).wait()
    rank, vecs = leaf_buf.shape[1:]
    leaf_out = leaf_out + dot(
        couple[...].reshape(REACH * band * rank, rank),
        leaf_buf[...].reshape(REACH * band * rank, vecs),
        ((0,), (0,)),
    )
    total = total + dot(leaf_out.astype(BF16), basis_row[...], ((0,), (0,)))
    out_ref[...] = total.astype(out_ref.dtype)

    for copy in near.values():
        copy.wait_send()
    pltpu.make_async_copy(region_buf, region_buf, group_sems.at[0]).wait()
    pltpu.make_async_copy(leaf_buf, leaf_buf, group_sems.at[2]).wait()


def per_device(
    vectors,
    near_blocks,
    near_source,
    near_count,
    basis_col,
    transfer_col,
    leaf_couple,
    coupling,
    distant_region_list,
    transfer_row,
    basis_row,
):
    rows, cols = lax.axis_size("row"), lax.axis_size("col")
    vecs, leaf = vectors.shape[2:]
    rank = basis_col.shape[2]
    cells = near_blocks.shape[2]
    band = leaf_couple.shape[3]
    smem = pl.BlockSpec(memory_space=pltpu.SMEM)
    hbm = pl.BlockSpec(memory_space=pl.ANY)
    out = pl.pallas_call(
        functools.partial(kernel, rows, cols),
        out_shape=jax.ShapeDtypeStruct((vecs, leaf), BF16),
        in_specs=[smem] * 3 + [hbm] * 8,
        out_specs=pl.BlockSpec(memory_space=pltpu.VMEM),
        scratch_shapes=[
            pltpu.VMEM((cells, vecs, leaf), BF16),
            pltpu.VMEM((cells, leaf, leaf), BF16),
            pltpu.VMEM((rank, leaf), BF16),
            pltpu.VMEM((rank, rank), BF16),
            pltpu.VMEM((REACH * band, rank, rank), BF16),
            pltpu.VMEM((rows, rank, rank), BF16),
            pltpu.VMEM((rank, rank), BF16),
            pltpu.VMEM((rank, leaf), BF16),
            pltpu.VMEM((rank, vecs), BF16),
            pltpu.VMEM((rank, vecs), BF16),
            pltpu.VMEM((REACH * band, rank, vecs), BF16),
            pltpu.VMEM(((rows - REACH) * cols, rank, vecs), BF16),
            pltpu.SemaphoreType.DMA((8,)),
            pltpu.SemaphoreType.DMA((cells,)),
            pltpu.SemaphoreType.DMA((cells,)),
            pltpu.SemaphoreType.DMA((4,)),
        ],
        compiler_params=pltpu.CompilerParams(collective_id=0, has_side_effects=True),
    )(
        near_source[0, 0],
        near_count,
        distant_region_list[0],
        vectors[0, 0],
        near_blocks[0, 0],
        basis_col[0, 0],
        transfer_col[0, 0],
        leaf_couple[0, 0].reshape(REACH * band, rank, rank),
        coupling[0],
        transfer_row[0, 0],
        basis_row[0, 0],
    )
    return out[None, None]


def solution(mesh):
    placed = (
        P("row", "col", None, None),
        P("row", "col", None, None, None),
        P("row", "col", None),
        P("row", "col"),
        P("row", "col", None, None),
        P("row", "col", None, None),
        P("row", "col", None, None, None, None),
        P("row", None, None, None),
        P("row", None),
        P("row", "col", None, None),
        P("row", "col", None, None),
    )
    return jax.shard_map(
        per_device,
        mesh=mesh,
        in_specs=placed,
        out_specs=P("row", "col", None, None),
        check_vma=False,
    )
```

```python
import functools

import jax
import jax.numpy as jnp
from jax import lax
from jax.experimental import pallas as pl
from jax.experimental.pallas import tpu as pltpu
from jax.sharding import PartitionSpec as P

REACH = 3
MESH = pl.DeviceIdType.MESH
BF16 = jnp.bfloat16
F32 = jnp.float32


def dot(a, b, dims):
    return lax.dot_general(a, b, (dims, ((), ())), preferred_element_type=F32)


def kernel(
    rows,
    cols,
    source_ref,
    count_ref,
    list_ref,
    vectors_hbm,
    blocks_hbm,
    basis_col_hbm,
    transfer_col_hbm,
    couple_hbm,
    coupling_hbm,
    transfer_row_hbm,
    basis_row_hbm,
    out_ref,
    table,
    blocks,
    basis_col,
    transfer_col,
    couple,
    coupling,
    transfer_row,
    basis_row,
    leaf_send,
    up_send,
    reduced_send,
    leaf_buf,
    chunk_buf,
    region_buf,
    local_sems,
    near_send_sems,
    near_recv_sems,
    group_sems,
):
    r, c = lax.axis_index("row"), lax.axis_index("col")
    band = cols - REACH

    def behind(d, e):
        return (lax.rem(r + rows - d, rows), lax.rem(c + cols - e, cols))

    barrier = pltpu.get_barrier_semaphore()
    if rows * cols <= 64:
        for k in range(1, rows * cols):
            pl.semaphore_signal(barrier, inc=1, device_id=behind(k // cols, k % cols), device_id_type=MESH)
    else:

        @pl.loop(1, rows * cols)
        def _(k):
            pl.semaphore_signal(
                barrier, inc=1, device_id=behind(k // cols, lax.rem(k, cols)), device_id_type=MESH
            )

    loads = [
        pltpu.make_async_copy(src, dst, local_sems.at[i])
        for i, (src, dst) in enumerate(
            [
                (vectors_hbm, table.at[0]),
                (basis_col_hbm, basis_col),
                (transfer_col_hbm, transfer_col),
                (blocks_hbm, blocks),
                (couple_hbm, couple),
                (coupling_hbm, coupling),
                (transfer_row_hbm, transfer_row),
                (basis_row_hbm, basis_row),
            ]
        )
    ]
    for load in loads:
        load.start()
    for load in loads[:3]:
        load.wait()
    leaf_low = dot(basis_col[...], table[0], ((1,), (1,))).astype(BF16)
    leaf_send[...] = leaf_low
    up = dot(transfer_col[...], leaf_low, ((0,), (0,))).astype(BF16)
    chunk = up_send.shape[1]
    for e in range(cols):
        up_send[e] = up[e * chunk : (e + 1) * chunk]

    pl.semaphore_wait(barrier, rows * cols - 1)

    def remote(src, dst, send_sem, recv_sem, target):
        return pltpu.make_async_remote_copy(
            src_ref=src, dst_ref=dst, send_sem=send_sem, recv_sem=recv_sem,
            device_id=target, device_id_type=MESH,
        )

    parity = lax.rem(r, 2)
    partner = (r + 1 - 2 * parity, c)
    odd, even = parity == 1, parity == 0

    for e in range(1, cols):
        remote(
            up_send.at[lax.rem(c + cols - e, cols)], chunk_buf.at[e], group_sems.at[0], group_sems.at[1], behind(0, e)
        ).start()
    own_band = leaf_buf.at[pl.ds(0, band)]
    mid_band = leaf_buf.at[pl.ds(band, band)]
    top_band = leaf_buf.at[pl.ds(2 * band, band)]
    for j in range(band):
        remote(leaf_send, leaf_buf.at[j], group_sems.at[2], group_sems.at[3], behind(0, REACH + j)).start()
    near = {}
    for d, e in ((2, 0), (0, 2), (0, 1), (2, 1), (2, 2)):
        cell = d * REACH + e
        near[cell] = remote(
            table.at[0], table.at[cell], near_send_sems.at[cell], near_recv_sems.at[cell], behind(d, e)
        )
        near[cell].start()
    for e in range(REACH):
        cell = REACH + e
        near[cell] = remote(
            table.at[2 * REACH * (1 - parity) + e],
            table.at[cell],
            near_send_sems.at[cell],
            near_recv_sems.at[cell],
            partner,
        )
    band_up = remote(own_band, top_band, group_sems.at[4], group_sems.at[5], behind(2, 0))
    band_across = remote(
        leaf_buf.at[pl.ds(2 * band * (1 - parity), band)], mid_band, group_sems.at[6], group_sems.at[7], partner
    )

    def start_if(condition, copy):
        @pl.when(condition)
        def _():
            copy.start()

    start_if(odd, near[REACH])
    for load in loads[3:]:
        load.wait()

    count = count_ref[0, 0]

    def term(cell):
        slot = jnp.int32(0)
        for s in range(source_ref.shape[0]):
            slot = jnp.where(source_ref[s] == cell, s, slot)
        source = table[cell]
        source = jnp.where(slot < count, source, jnp.zeros_like(source))
        return dot(source, blocks[slot], ((1,), (0,)))

    arrived = chunk_buf.at[pl.ds(1, cols - 1)]
    pltpu.make_async_copy(arrived, arrived, group_sems.at[1]).wait()
    reduced = up_send[c].astype(F32)
    for e in range(1, cols):
        reduced = reduced + chunk_buf[e].astype(F32)
    reduced_send[...] = reduced.astype(BF16)
    pltpu.make_async_copy(own_band, own_band, group_sems.at[3]).wait()
    band_up.start()
    start_if(odd, band_across)
    total = term(0)
    for d in range(REACH, rows):
        for e in range(cols):
            remote(
                reduced_send, region_buf.at[d - REACH, c], group_sems.at[8], group_sems.at[9], behind(d, e)
            ).start()

    near[2 * REACH].wait_recv()
    start_if(even, near[REACH])
    total = total + term(2 * REACH)
    band_up.wait_recv()
    start_if(even, band_across)
    for e in (2, 1):
        near[e].wait_recv()
        start_if(odd, near[REACH + e])
        total = total + term(e)
    near[REACH].wait_recv()
    total = total + term(REACH)

    pltpu.make_async_copy(region_buf, region_buf, group_sems.at[9]).wait()
    rank, vecs = leaf_buf.shape[1:]
    region_out = None
    for d in range(REACH, rows):
        target = lax.rem(r + d, rows)
        slot = jnp.int32(0)
        for f in range(rows):
            slot = jnp.where(list_ref[f] == target, f, slot)
        region = region_buf[d - REACH].astype(F32).reshape(rank, vecs).astype(BF16)
        part = dot(coupling[slot], region, ((0,), (0,)))
        region_out = part if region_out is None else region_out + part
    leaf_out = dot(transfer_row[...], region_out.astype(BF16), ((0,), (0,)))
    band_across.wait_recv()
    leaf_out = leaf_out + dot(
        couple[...].reshape(REACH * band * rank, rank),
        leaf_buf[...].reshape(REACH * band * rank, vecs),
        ((0,), (0,)),
    )
    total = total + dot(leaf_out.astype(BF16), basis_row[...], ((0,), (0,)))

    for e in (1, 2):
        near[2 * REACH + e].wait_recv()
        start_if(even, near[REACH + e])
        total = total + term(2 * REACH + e)
    for e in (1, 2):
        near[REACH + e].wait_recv()
        total = total + term(REACH + e)
    out_ref[...] = total.astype(out_ref.dtype)

    for copy in near.values():
        copy.wait_send()
    band_up.wait_send()
    band_across.wait_send()
    pltpu.make_async_copy(arrived, arrived, group_sems.at[0]).wait()
    pltpu.make_async_copy(own_band, own_band, group_sems.at[2]).wait()
    pltpu.make_async_copy(region_buf, region_buf, group_sems.at[8]).wait()


def per_device(
    vectors,
    near_blocks,
    near_source,
    near_count,
    basis_col,
    transfer_col,
    leaf_couple,
    coupling,
    distant_region_list,
    transfer_row,
    basis_row,
):
    rows, cols = lax.axis_size("row"), lax.axis_size("col")
    vecs, leaf = vectors.shape[2:]
    rank = basis_col.shape[2]
    cells = near_blocks.shape[2]
    band = leaf_couple.shape[3]
    smem = pl.BlockSpec(memory_space=pltpu.SMEM)
    hbm = pl.BlockSpec(memory_space=pl.ANY)
    out = pl.pallas_call(
        functools.partial(kernel, rows, cols),
        out_shape=jax.ShapeDtypeStruct((vecs, leaf), BF16),
        in_specs=[smem] * 3 + [hbm] * 8,
        out_specs=pl.BlockSpec(memory_space=pltpu.VMEM),
        scratch_shapes=[
            pltpu.VMEM((cells, vecs, leaf), BF16),
            pltpu.VMEM((cells, leaf, leaf), BF16),
            pltpu.VMEM((rank, leaf), BF16),
            pltpu.VMEM((rank, rank), BF16),
            pltpu.VMEM((REACH * band, rank, rank), BF16),
            pltpu.VMEM((rows, rank, rank), BF16),
            pltpu.VMEM((rank, rank), BF16),
            pltpu.VMEM((rank, leaf), BF16),
            pltpu.VMEM((rank, vecs), BF16),
            pltpu.VMEM((cols, rank // cols, vecs), BF16),
            pltpu.VMEM((rank // cols, vecs), BF16),
            pltpu.VMEM((REACH * band, rank, vecs), BF16),
            pltpu.VMEM((cols, rank // cols, vecs), BF16),
            pltpu.VMEM((rows - REACH, cols, rank // cols, vecs), BF16),
            pltpu.SemaphoreType.DMA((8,)),
            pltpu.SemaphoreType.DMA((cells,)),
            pltpu.SemaphoreType.DMA((cells,)),
            pltpu.SemaphoreType.DMA((10,)),
        ],
        compiler_params=pltpu.CompilerParams(collective_id=0, has_side_effects=True),
    )(
        near_source[0, 0],
        near_count,
        distant_region_list[0],
        vectors[0, 0],
        near_blocks[0, 0],
        basis_col[0, 0],
        transfer_col[0, 0],
        leaf_couple[0, 0].reshape(REACH * band, rank, rank),
        coupling[0],
        transfer_row[0, 0],
        basis_row[0, 0],
    )
    return out[None, None]


def solution(mesh):
    placed = (
        P("row", "col", None, None),
        P("row", "col", None, None, None),
        P("row", "col", None),
        P("row", "col"),
        P("row", "col", None, None),
        P("row", "col", None, None),
        P("row", "col", None, None, None, None),
        P("row", None, None, None),
        P("row", None),
        P("row", "col", None, None),
        P("row", "col", None, None),
    )
    return jax.shard_map(
        per_device,
        mesh=mesh,
        in_specs=placed,
        out_specs=P("row", "col", None, None),
        check_vma=False,
    )
```
